32 devices in a mesh: chan: 2 (over x), vis: 2 (over core), pix: 8 (over z, y).
Axes of the slice: x: 2, y: 2, z: 4, core: 2. Of those that a mesh axis runs over, the one named last changes fastest.
Arguments:
- response: bfloat16 [16384, 49152], P(('chan', 'vis'), 'pix'), parts along dimension 0, may hold values from -5 to 5
- vis_data: float32 [16384], P(('chan', 'vis')), parts along dimension 0, may hold values from -6 to 6
- baseline_of_row: int32 [8192], P('vis'), may hold values from 0 to 8191
- noise_class: int32 [8192], P('vis'), may hold values from 0 to 15
- baseline_weight: float32 [8192], replicated, may hold values from 0.25 to 4
- class_inv_var: float32 [32], P('chan'), parts along dimension 0, may hold values from 0.25 to 4
Outputs:
- sky_map: float32 [98304], P(('chan', 'pix')), parts along dimension 0
- psf: float32 [98304, 64], P(('chan', 'pix'), 'vis'), parts along dimension 0
The draws below stay inside these ranges and needn't reach their ends.
There are 2 independent parts, one for each index of `chan`. The reference program is written for one: setup_inputs(seed, part) draws one part's arguments, and reference() takes and returns one part's arrays. A program takes and returns all parts, laid end to end along the dimension named above; an argument that names none is the same for every part. Nothing has to cross between parts.
Inputs may be any that keep to these rules, and one draw needn't show every extreme that they name: `baseline_of_row`: baseline index of each row.
All inputs are finite; a program needn't handle non-finite values.
Results may differ from the reference program's by a relative error of at most 0.0041.
Values may be sent and summed in bfloat16 or wider, within the bound.
No kernel may reach another device: no remote copies, remote signals or barrier semaphores. Data moves between devices by JAX's collectives and lax.ppermute only.
A program may use at most 128 MiB of HBM per device.

```python
import math
import jax
import jax.numpy as jnp
from jax import lax

PIX = 49152
PANEL_DEV = 8
NBL = 8192
NCLASS = 16
VIS = 8192
N_PIX = 8


def with_ends(entries, stream_key, smallest, largest):
    place = [jax.random.randint(jax.random.fold_in(stream_key, axis), (), 0, length) for axis, length in enumerate(entries.shape)]
    longest = entries.shape.index(max(entries.shape))
    beside = place[:longest] + [(place[longest] + 1) % entries.shape[longest]] + place[longest + 1:]
    return entries.at[tuple(place)].set(smallest).at[tuple(beside)].set(largest)


def steps_of(own_key, dims, shards, least, top_value):
    def one(axis_at, parts):
        draws = jax.random.uniform(jax.random.fold_in(jax.random.fold_in(own_key, 6), axis_at), (parts,), jnp.float32, least / len(shards), top_value / len(shards))
        return jnp.repeat(jnp.exp(draws), dims[axis_at] // parts).reshape((-1,) + (1,) * (len(dims) - axis_at - 1))

    gain = one(*shards[0])
    for cut in shards[1:]:
        gain = gain * one(*cut)
    return gain


def noise(key, extent, spread, limit, cuts=(), held_as=jnp.bfloat16):
    loudness = steps_of(key, extent, cuts, -0.22, 0.18) if cuts else 1.0
    result = jax.random.normal(key, extent, jnp.float32) * spread * loudness
    return jnp.minimum(jnp.maximum(result, -limit), limit).astype(held_as)


def setup_inputs(seed: int = 0, part: int = 0) -> dict:
    seeds = jax.random.split(jax.random.key(seed), 7)
    part_keys = jax.random.split(jax.random.fold_in(seeds[6], part), 7)
    return {
        "response": noise(part_keys[0], (VIS, PIX), 1.0, 5.0, ((0, 2), (1, 8))),
        "vis_data": noise(part_keys[1], (VIS,), 1.0, 6.0, ((0, 2),), jnp.float32),
        "baseline_of_row": with_ends(jax.random.randint(seeds[2], (VIS,), 0, NBL), jax.random.fold_in(seeds[2], 1), 0, NBL - 1).astype(jnp.int32),
        "noise_class": with_ends(jax.random.randint(seeds[3], (VIS,), 0, NCLASS), jax.random.fold_in(seeds[3], 1), 0, NCLASS - 1).astype(jnp.int32),
        "baseline_weight": jnp.clip(jnp.exp(jax.random.uniform(seeds[4], (NBL,), jnp.float32, math.log(0.25), math.log(4.0))), 0.25, 4.0),
        "class_inv_var": jnp.clip(jnp.exp(jax.random.uniform(part_keys[5], (NCLASS,), jnp.float32, math.log(0.25), math.log(4.0))), 0.25, 4.0),
    }


def add_norm(total, pair):
    resp_block, weight_block = pair
    squares = jnp.square(resp_block.astype(jnp.float32))
    return (total + lax.optimization_barrier(jnp.sum(weight_block[:, None] * squares, axis=0)), None)

def reference(response, vis_data, baseline_of_row, noise_class, baseline_weight, class_inv_var):
    weight_row = baseline_weight[baseline_of_row] * class_inv_var[noise_class]
    pix_block = PIX // N_PIX
    blocks = response.reshape(VIS, N_PIX, pix_block)
    panel_cols = blocks[:, :, :PANEL_DEV].reshape(VIS, N_PIX * PANEL_DEV)
    weighted_panel = (weight_row[:, None] * panel_cols.astype(jnp.float32)).astype(jnp.bfloat16)
    weighted_vis = (weight_row * vis_data).astype(jnp.bfloat16)
    dirty_map = jnp.dot(weighted_vis, response, preferred_element_type=jnp.float32)
    row_step = math.gcd(VIS, 512)
    stacked = response.reshape(VIS // row_step, row_step, PIX)
    stacked_weight = weight_row.reshape(VIS // row_step, row_step)
    pixel_norm, unused = lax.scan(add_norm, jnp.zeros((PIX,), jnp.float32), (stacked, stacked_weight))
    beam_full = jnp.dot(response.T, weighted_panel, preferred_element_type=jnp.float32)
    panel_norm = pixel_norm.reshape(N_PIX, pix_block)[:, :PANEL_DEV].reshape(N_PIX * PANEL_DEV)
    sky_map = dirty_map / jnp.sqrt(pixel_norm)
    psf = beam_full / jnp.sqrt(pixel_norm[:, None] * panel_norm[None, :])
    return (sky_map, psf)
```

```python
import functools

import jax
import jax.numpy as jnp
from jax import lax
from jax.experimental import pallas as pl
from jax.experimental.pallas import tpu as pltpu
from jax.sharding import PartitionSpec as P

PANEL_DEV = 8
LANES = 128
ROWS = 16
KEPT_FRACTION = 0.5
ANY = pl.BlockSpec(memory_space=pl.ANY)
VMEM = pl.BlockSpec(memory_space=pltpu.VMEM)
SMEM = pl.BlockSpec(memory_space=pltpu.SMEM)


def square_sums(rows, block, first, width):
    depth = rows.shape[1]
    step = min(depth, 1024)
    total = None
    for at in range(0, depth, step):
        part = block[pl.ds(at, step), pl.ds(first, width)]
        term = jnp.dot(rows[:, at : at + step], part * part, preferred_element_type=jnp.float32)
        total = term if total is None else total + term
    return total[1:2] + total[2:3]


def copies_of(source, first, target, sems, width, count):
    def one(c):
        start = pl.multiple_of(c * width, width)
        return pltpu.make_async_copy(
            source.at[:, pl.ds(pl.multiple_of(first + start, LANES), width)],
            target.at[:, pl.ds(start, width)],
            sems.at[c],
        )

    return one


def head(width, count, class_ref, base_ref, noise_ref, vis_ref, table_ref, response,
         kept, rows_out, weight_out, norm_out, sems):
    copy = copies_of(response, 0, kept, sems, width, count)
    for c in range(count):
        copy(c).start()
    base = base_ref[...]
    lane = jnp.bitwise_and(base, LANES - 1)
    line = jnp.right_shift(base, 7)
    weight = jnp.zeros(base.shape, jnp.float32)
    for t in range(table_ref.shape[0]):
        entries = jnp.broadcast_to(table_ref[t : t + 1, :], base.shape)
        found = jnp.take_along_axis(entries, lane, axis=1, mode="promise_in_bounds")
        weight = jnp.where(line == t, found, weight)
    noise = noise_ref[...]
    scale = jnp.zeros(base.shape, jnp.float32)
    for t in range(class_ref.shape[0]):
        scale = jnp.where(noise == t, class_ref[t], scale)
    weight = weight * scale
    weight_out[...] = weight
    weighted_vis = weight * vis_ref[...]
    high = weight.astype(jnp.bfloat16).astype(jnp.float32)
    low = weight - high
    place = lax.broadcasted_iota(jnp.int32, (ROWS, LANES), 0)
    for s in range(base.shape[0]):
        piece = jnp.where(place == 0, weighted_vis[s : s + 1], 0.0)
        piece = jnp.where(place == 1, high[s : s + 1], piece)
        piece = jnp.where(place == 2, low[s : s + 1], piece)
        rows_out[:, s * LANES : (s + 1) * LANES] = piece.astype(jnp.bfloat16)

    def body(c, carry):
        copy(c).wait()
        first = pl.multiple_of(c * width, width)
        norm_out[:, pl.ds(first, width)] = square_sums(rows_out[...], kept, first, width)
        return carry

    lax.fori_loop(0, count, body, 0)


def tail(width, kept_count, count, groups, slot_ref, *refs):
    panels = refs[:groups]
    kept, rows_ref, weight_ref, norm_ref, response, keep, send, stage, lhs, rest, sems = refs[groups:]
    n = stage.shape[0]
    half = n // 2
    used = kept_count * width
    columns = response.shape[1]
    copy = copies_of(response, used, rest, sems, width, count)
    for c in range(count):
        copy(c).start()
    per = panels[0].shape[0] // PANEL_DEV
    for g in range(groups):
        for i in range(per):
            slot = slot_ref[g * per + i]
            panel = panels[g][i * PANEL_DEV : (i + 1) * PANEL_DEV, :].astype(jnp.float32)
            for s in range(weight_ref.shape[0]):
                cols = slice(s * LANES, (s + 1) * LANES)
                stage[slot, :, cols] = panel[:, cols] * weight_ref[s : s + 1, :]
            total = jnp.zeros((PANEL_DEV, LANES), jnp.float32)
            for s in range(weight_ref.shape[0]):
                cols = slice(s * LANES, (s + 1) * LANES)
                total = total + panel[:, cols] * panel[:, cols] * weight_ref[s : s + 1, :]
            own = jnp.broadcast_to(jnp.sum(total, axis=1, keepdims=True), (PANEL_DEV, LANES))

            def put(out, at):
                out[pl.ds(pl.multiple_of(at * PANEL_DEV, PANEL_DEV), PANEL_DEV), columns:] = own

            @pl.when(slot < half)
            def _():
                put(keep, slot)

            @pl.when(slot >= half)
            def _():
                put(send, slot - half)

    for k in range(0, n, 2):
        pair = jnp.concatenate([stage[k], stage[k + 1]], axis=0)
        lhs[k * PANEL_DEV : (k + 2) * PANEL_DEV, :] = pair.astype(jnp.bfloat16)
    lhs[n * PANEL_DEV :, :] = rows_ref[...]
    share = half * PANEL_DEV
    place = lax.broadcasted_iota(jnp.int32, (PANEL_DEV, width), 0)
    extra = jnp.zeros((PANEL_DEV, LANES), jnp.float32)
    keep[share:, columns:] = extra
    send[share:, columns:] = extra

    def emit(block, first, out_first, norm):
        result = jnp.dot(
            lhs[...], block[:, pl.ds(first, width)], preferred_element_type=jnp.float32
        )
        dirty = result[2 * share : 2 * share + 1]
        both = jnp.where(place == 0, dirty, jnp.where(place == 1, norm, 0.0))
        out = pl.ds(out_first, width)
        keep[:share, out] = result[:share]
        send[:share, out] = result[share : 2 * share]
        keep[share:, out] = both
        send[share:, out] = both

    def early(c, carry):
        first = pl.multiple_of(c * width, width)
        emit(kept, first, first, norm_ref[:, pl.ds(first, width)])
        return carry

    lax.fori_loop(0, kept_count, early, 0)

    def late(c, carry):
        copy(c).wait()
        first = pl.multiple_of(c * width, width)
        norm = square_sums(rows_ref[...], rest, first, width)
        emit(rest, first, pl.multiple_of(used + first, LANES), norm)
        return carry

    lax.fori_loop(0, count, late, 0)


def finish(keep, got, sky, psf):
    columns = sky.shape[1]
    share = psf.shape[0]
    total = keep[share : share + 2, :columns] + got[share : share + 2, :columns]
    scale = lax.rsqrt(total[1:2])
    sky[...] = total[0:1] * scale
    panel = lax.rsqrt(keep[:share, columns:] + got[:share, columns:])[:, :1]
    step = next(w for w in (512, 256, 128) if columns % w == 0)
    for at in range(0, columns, step):
        cols = slice(at, at + step)
        psf[:, cols] = (keep[:share, cols] + got[:share, cols]) * scale[:, cols] * panel


def gather_panels(own):
    n = lax.axis_size("pix")
    inner = next(w for w in (8, 4, 2, 1) if n % w == 0)
    blocks = [own]
    for step in range(1, inner):
        pairs = [(k, k // inner * inner + (k + step) % inner) for k in range(n)]
        blocks.append(lax.ppermute(own, "pix", pairs))
    me = lax.axis_index("pix")
    place = [(me // inner * inner + (me % inner - step) % inner) for step in range(inner)]
    if n > inner:
        near = jnp.concatenate(blocks, axis=0)
        blocks = [near]
        outer = n // inner
        sources = list(place)
        for step in range(1, outer):
            pairs = [(k, (k + step * inner) % n) for k in range(n)]
            blocks.append(lax.ppermute(near, "pix", pairs))
            sources += [(p - step * inner) % n for p in place]
        place = sources
    return blocks, jnp.stack(place)


def shards(response, vis_data, baseline_of_row, noise_class, baseline_weight, class_inv_var):
    depth, columns = response.shape
    n = lax.axis_size("pix")
    half = n // 2
    width = 512 if columns % 512 == 0 else 256
    chunks = columns // width
    kept_count = max(1, int(chunks * KEPT_FRACTION))
    count = chunks - kept_count
    own = response[:, :PANEL_DEV].T
    panels, source = gather_panels(own)
    vis = lax.axis_index("vis")
    slots = jnp.where(source // half == vis, source % half, half + source % half).astype(jnp.int32)

    as_lines = lambda x: x.reshape(-1, LANES)
    lines = depth // LANES
    head_width = kept_count * width
    kept, rows, weight, norm = pl.pallas_call(
        functools.partial(head, width, kept_count),
        out_shape=(
            pltpu.VMEM((depth, head_width), jnp.bfloat16),
            jax.ShapeDtypeStruct((ROWS, depth), jnp.bfloat16),
            jax.ShapeDtypeStruct((lines, LANES), jnp.float32),
            jax.ShapeDtypeStruct((1, head_width), jnp.float32),
        ),
        in_specs=[SMEM, VMEM, VMEM, VMEM, VMEM, ANY],
        out_specs=(VMEM,) * 4,
        scratch_shapes=[pltpu.SemaphoreType.DMA((kept_count,))],
        compiler_params=pltpu.CompilerParams(vmem_limit_bytes=10 << 20),
        cost_estimate=pl.CostEstimate(
            flops=64 * depth * head_width, bytes_accessed=2 * depth * head_width, transcendentals=0
        ),
        name="head",
    )(class_inv_var, as_lines(baseline_of_row), as_lines(noise_class), as_lines(vis_data),
      as_lines(baseline_weight), response)

    share = half * PANEL_DEV
    kept = pltpu.with_memory_space_constraint(kept, pltpu.VMEM)
    part = jax.ShapeDtypeStruct((share + PANEL_DEV, columns + LANES), jnp.float32)
    keep, send = pl.pallas_call(
        functools.partial(tail, width, kept_count, count, len(panels)),
        out_shape=(part, part),
        in_specs=[SMEM] + [VMEM] * len(panels) + [VMEM] * 4 + [ANY],
        out_specs=(VMEM, VMEM),
        scratch_shapes=[
            pltpu.VMEM((n, PANEL_DEV, depth), jnp.float32),
            pltpu.VMEM((n * PANEL_DEV + ROWS, depth), jnp.bfloat16),
            pltpu.VMEM((depth, count * width), jnp.bfloat16),
            pltpu.SemaphoreType.DMA((count,)),
        ],
        compiler_params=pltpu.CompilerParams(vmem_limit_bytes=30 << 20),
        cost_estimate=pl.CostEstimate(
            flops=2 * depth * columns * (n * PANEL_DEV), bytes_accessed=2 * depth * columns,
            transcendentals=0,
        ),
        name="tail",
    )(slots, *panels, kept, rows, weight, norm, response)
    got = lax.ppermute(send, "vis", [(0, 1), (1, 0)])
    sky, psf = pl.pallas_call(
        finish,
        out_shape=(
            jax.ShapeDtypeStruct((1, columns), jnp.float32),
            jax.ShapeDtypeStruct((share, columns), jnp.float32),
        ),
        in_specs=[VMEM, VMEM],
        out_specs=(VMEM, VMEM),
        compiler_params=pltpu.CompilerParams(vmem_limit_bytes=16 << 20),
        name="finish",
    )(keep, got)
    return sky.reshape(-1), psf.T


def solution(mesh):
    placed = (P(("chan", "vis"), "pix"), P(("chan", "vis")), P("vis"), P("vis"), P(), P("chan"))
    return jax.shard_map(
        shards,
        mesh=mesh,
        in_specs=placed,
        out_specs=(P(("chan", "pix")), P(("chan", "pix"), "vis")),
        check_vma=False,
    )
```

```python
import functools

import jax
import jax.numpy as jnp
from jax import lax
from jax.experimental import pallas as pl
from jax.experimental.pallas import tpu as pltpu
from jax.sharding import PartitionSpec as P

PANEL_DEV = 8
LANES = 128
ROWS = 16
KEPT_FRACTION = 0.34
ANY = pl.BlockSpec(memory_space=pl.ANY)
VMEM = pl.BlockSpec(memory_space=pltpu.VMEM)
SMEM = pl.BlockSpec(memory_space=pltpu.SMEM)


def square_sums(rows, block, first, width):
    depth = rows.shape[1]
    step = min(depth, 1024)
    total = None
    for at in range(0, depth, step):
        part = block[pl.ds(at, step), pl.ds(first, width)]
        term = jnp.dot(rows[:, at : at + step], part * part, preferred_element_type=jnp.float32)
        total = term if total is None else total + term
    return total[1:2] + total[2:3]


def copies_of(source, first, target, sems, width, count):
    def one(c):
        start = pl.multiple_of(c * width, width)
        return pltpu.make_async_copy(
            source.at[:, pl.ds(pl.multiple_of(first + start, LANES), width)],
            target.at[:, pl.ds(start, width)],
            sems.at[c],
        )

    return one


def head(width, count, class_ref, base_ref, noise_ref, vis_ref, table_ref, response,
         kept, rows_out, weight_out, norm_out, sems):
    copy = copies_of(response, 0, kept, sems, width, count)
    for c in range(count):
        copy(c).start()
    base = base_ref[...]
    lane = jnp.bitwise_and(base, LANES - 1)
    line = jnp.right_shift(base, 7)
    weight = jnp.zeros(base.shape, jnp.float32)
    for t in range(table_ref.shape[0]):
        entries = jnp.broadcast_to(table_ref[t : t + 1, :], base.shape)
        found = jnp.take_along_axis(entries, lane, axis=1, mode="promise_in_bounds")
        weight = jnp.where(line == t, found, weight)
    noise = noise_ref[...]
    scale = jnp.zeros(base.shape, jnp.float32)
    for t in range(class_ref.shape[0]):
        scale = jnp.where(noise == t, class_ref[t], scale)
    weight = weight * scale
    weight_out[...] = weight
    weighted_vis = weight * vis_ref[...]
    high = weight.astype(jnp.bfloat16).astype(jnp.float32)
    low = weight - high
    place = lax.broadcasted_iota(jnp.int32, (ROWS, LANES), 0)
    for s in range(base.shape[0]):
        piece = jnp.where(place == 0, weighted_vis[s : s + 1], 0.0)
        piece = jnp.where(place == 1, high[s : s + 1], piece)
        piece = jnp.where(place == 2, low[s : s + 1], piece)
        rows_out[:, s * LANES : (s + 1) * LANES] = piece.astype(jnp.bfloat16)

    def body(c, carry):
        copy(c).wait()
        first = pl.multiple_of(c * width, width)
        norm_out[:, pl.ds(first, width)] = square_sums(rows_out[...], kept, first, width)
        return carry

    lax.fori_loop(0, count, body, 0)


def tail(width, kept_count, count, groups, slot_ref, *refs):
    panels = refs[:groups]
    kept, rows_ref, weight_ref, norm_ref, response, keep, send, stage, lhs, rest, sems = refs[groups:]
    n = stage.shape[0]
    half = n // 2
    used = kept_count * width
    columns = response.shape[1]
    copy = copies_of(response, used, rest, sems, width, count)
    for c in range(count):
        copy(c).start()
    per = panels[0].shape[0] // PANEL_DEV
    for g in range(groups):
        for i in range(per):
            slot = slot_ref[g * per + i]
            panel = panels[g][i * PANEL_DEV : (i + 1) * PANEL_DEV, :].astype(jnp.float32)
            for s in range(weight_ref.shape[0]):
                cols = slice(s * LANES, (s + 1) * LANES)
                stage[slot, :, cols] = panel[:, cols] * weight_ref[s : s + 1, :]
            total = jnp.zeros((PANEL_DEV, LANES), jnp.float32)
            for s in range(weight_ref.shape[0]):
                cols = slice(s * LANES, (s + 1) * LANES)
                total = total + panel[:, cols] * panel[:, cols] * weight_ref[s : s + 1, :]
            own = jnp.broadcast_to(jnp.sum(total, axis=1, keepdims=True), (PANEL_DEV, LANES))

            def put(out, at):
                out[pl.ds(pl.multiple_of(at * PANEL_DEV, PANEL_DEV), PANEL_DEV), columns:] = own

            @pl.when(slot < half)
            def _():
                put(keep, slot)

            @pl.when(slot >= half)
            def _():
                put(send, slot - half)

    for k in range(0, n, 2):
        pair = jnp.concatenate([stage[k], stage[k + 1]], axis=0)
        lhs[k * PANEL_DEV : (k + 2) * PANEL_DEV, :] = pair.astype(jnp.bfloat16)
    lhs[n * PANEL_DEV :, :] = rows_ref[...]
    share = half * PANEL_DEV
    place = lax.broadcasted_iota(jnp.int32, (PANEL_DEV, width), 0)
    extra = jnp.zeros((PANEL_DEV, LANES), jnp.float32)
    keep[share:, columns:] = extra
    send[share:, columns:] = extra

    def emit(block, first, out_first, norm):
        result = jnp.dot(
            lhs[...], block[:, pl.ds(first, width)], preferred_element_type=jnp.float32
        )
        dirty = result[2 * share : 2 * share + 1]
        both = jnp.where(place == 0, dirty, jnp.where(place == 1, norm, 0.0))
        out = pl.ds(out_first, width)
        keep[:share, out] = result[:share]
        send[:share, out] = result[share : 2 * share]
        keep[share:, out] = both
        send[share:, out] = both

    def early(c, carry):
        first = pl.multiple_of(c * width, width)
        emit(kept, first, first, norm_ref[:, pl.ds(first, width)])
        return carry

    lax.fori_loop(0, kept_count, early, 0)

    def late(c, carry):
        copy(c).wait()
        first = pl.multiple_of(c * width, width)
        norm = square_sums(rows_ref[...], rest, first, width)
        emit(rest, first, pl.multiple_of(used + first, LANES), norm)
        return carry

    lax.fori_loop(0, count, late, 0)


def finish(keep, got, sky, psf):
    columns = sky.shape[1]
    share = psf.shape[0]
    total = keep[share : share + 2, :columns] + got[share : share + 2, :columns]
    scale = lax.rsqrt(total[1:2])
    sky[...] = total[0:1] * scale
    panel = lax.rsqrt(keep[:share, columns:] + got[:share, columns:])[:, :1]
    step = next(w for w in (512, 256, 128) if columns % w == 0)
    for at in range(0, columns, step):
        cols = slice(at, at + step)
        psf[:, cols] = (keep[:share, cols] + got[:share, cols]) * scale[:, cols] * panel


def gather_panels(own):
    n = lax.axis_size("pix")
    inner = next(w for w in (8, 4, 2, 1) if n % w == 0)
    blocks = [own]
    for step in range(1, inner):
        pairs = [(k, k // inner * inner + (k + step) % inner) for k in range(n)]
        blocks.append(lax.ppermute(own, "pix", pairs))
    me = lax.axis_index("pix")
    place = [(me // inner * inner + (me % inner - step) % inner) for step in range(inner)]
    if n > inner:
        near = jnp.concatenate(blocks, axis=0)
        blocks = [near]
        outer = n // inner
        sources = list(place)
        for step in range(1, outer):
            pairs = [(k, (k + step * inner) % n) for k in range(n)]
            blocks.append(lax.ppermute(near, "pix", pairs))
            sources += [(p - step * inner) % n for p in place]
        place = sources
    return blocks, jnp.stack(place)


def shards(response, vis_data, baseline_of_row, noise_class, baseline_weight, class_inv_var):
    depth, columns = response.shape
    n = lax.axis_size("pix")
    half = n // 2
    width = 512 if columns % 512 == 0 else 256
    chunks = columns // width
    kept_count = max(1, int(chunks * KEPT_FRACTION))
    count = chunks - kept_count
    own = response[:, :PANEL_DEV].T
    panels, source = gather_panels(own)
    vis = lax.axis_index("vis")
    slots = jnp.where(source // half == vis, source % half, half + source % half).astype(jnp.int32)

    as_lines = lambda x: x.reshape(-1, LANES)
    lines = depth // LANES
    far = lambda x: pltpu.with_memory_space_constraint(x, pltpu.HBM)
    near = lambda x: pltpu.with_memory_space_constraint(x, pltpu.VMEM)
    head_width = kept_count * width
    kept, rows, weight, norm = pl.pallas_call(
        functools.partial(head, width, kept_count),
        out_shape=(
            pltpu.VMEM((depth, head_width), jnp.bfloat16),
            pltpu.VMEM((ROWS, depth), jnp.bfloat16),
            pltpu.VMEM((lines, LANES), jnp.float32),
            pltpu.VMEM((1, head_width), jnp.float32),
        ),
        in_specs=[SMEM, VMEM, VMEM, VMEM, VMEM, ANY],
        out_specs=(VMEM,) * 4,
        scratch_shapes=[pltpu.SemaphoreType.DMA((kept_count,))],
        compiler_params=pltpu.CompilerParams(vmem_limit_bytes=10 << 20),
        cost_estimate=pl.CostEstimate(
            flops=64 * depth * head_width, bytes_accessed=2 * depth * head_width, transcendentals=0
        ),
        name="head",
    )(class_inv_var, far(as_lines(baseline_of_row)), far(as_lines(noise_class)),
      far(as_lines(vis_data)), far(as_lines(baseline_weight)), response)

    share = half * PANEL_DEV
    kept, rows, weight, norm = map(near, (kept, rows, weight, norm))
    panels = [near(panel) for panel in panels]
    part = pltpu.VMEM((share + PANEL_DEV, columns + LANES), jnp.float32)
    keep, send = pl.pallas_call(
        functools.partial(tail, width, kept_count, count, len(panels)),
        out_shape=(part, part),
        in_specs=[SMEM] + [VMEM] * len(panels) + [VMEM] * 4 + [ANY],
        out_specs=(VMEM, VMEM),
        scratch_shapes=[
            pltpu.VMEM((n, PANEL_DEV, depth), jnp.float32),
            pltpu.VMEM((n * PANEL_DEV + ROWS, depth), jnp.bfloat16),
            pltpu.VMEM((depth, count * width), jnp.bfloat16),
            pltpu.SemaphoreType.DMA((count,)),
        ],
        compiler_params=pltpu.CompilerParams(vmem_limit_bytes=40 << 20),
        cost_estimate=pl.CostEstimate(
            flops=2 * depth * columns * (n * PANEL_DEV), bytes_accessed=2 * depth * columns,
            transcendentals=0,
        ),
        name="tail",
    )(slots, *panels, kept, rows, weight, norm, response)
    got = lax.ppermute(send, "vis", [(0, 1), (1, 0)])
    sky, psf = pl.pallas_call(
        finish,
        out_shape=(
            jax.ShapeDtypeStruct((1, columns), jnp.float32),
            jax.ShapeDtypeStruct((share, columns), jnp.float32),
        ),
        in_specs=[VMEM, VMEM],
        out_specs=(VMEM, VMEM),
        compiler_params=pltpu.CompilerParams(vmem_limit_bytes=16 << 20),
        name="finish",
    )(near(keep), near(got))
    return sky.reshape(-1), psf.T


def solution(mesh):
    placed = (P(("chan", "vis"), "pix"), P(("chan", "vis")), P("vis"), P("vis"), P(), P("chan"))
    return jax.shard_map(
        shards,
        mesh=mesh,
        in_specs=placed,
        out_specs=(P(("chan", "pix")), P(("chan", "pix"), "vis")),
        check_vma=False,
    )
```
